32 devices in a mesh: rows: 2 (over y), cols: 8 (over z, core), shift: 2 (over x).
Axes of the slice: x: 2, y: 2, z: 4, core: 2. Of those that a mesh axis runs over, the one named last changes fastest.
Arguments:
- train_gate: bfloat16 [7168, 14336], P(('shift', 'rows'), 'cols'), parts along dimension 0, may hold values from -0.09375 to 0.09375
- low_gate: bfloat16 [7168, 64], P(('shift', 'rows')), parts along dimension 0, may hold values from -0.09375 to 0.09375
- high_gate: bfloat16 [128, 14336], P('shift', 'cols'), parts along dimension 0, may hold values from -0.75 to 0.75
- train_up: bfloat16 [7168, 14336], P(('shift', 'rows'), 'cols'), parts along dimension 0, may hold values from -0.09375 to 0.09375
- low_up: bfloat16 [7168, 64], P(('shift', 'rows')), parts along dimension 0, may hold values from -0.09375 to 0.09375
- high_up: bfloat16 [128, 14336], P('shift', 'cols'), parts along dimension 0, may hold values from -0.75 to 0.75
- train_down: bfloat16 [28672, 3584], P(('shift', 'cols'), 'rows'), parts along dimension 0, may hold values from -0.046875 to 0.046875
- low_down: bfloat16 [28672, 64], P(('shift', 'cols')), parts along dimension 0, may hold values from -0.046875 to 0.046875
- high_down: bfloat16 [128, 3584], P('shift', 'rows'), parts along dimension 0, may hold values from -0.75 to 0.75
- norm_train: float32 [7168], P(('shift', 'rows', 'cols')), parts along dimension 0, may hold values from 0.25 to 1.75
- norm_step: float32 [7168], P(('shift', 'rows', 'cols')), parts along dimension 0, may hold values from -0.3 to 0.3
Outputs:
- serving_gate: bfloat16 [28672, 3584], P(('shift', 'cols')), parts along dimension 0
- serving_up: bfloat16 [28672, 3584], P(('shift', 'cols')), parts along dimension 0
- serving_down: bfloat16 [7168, 14336], P('shift', 'cols'), parts along dimension 0
- serve_norm: bfloat16 [7168], P('shift'), parts along dimension 0
The draws below stay inside these ranges and needn't reach their ends.
There are 2 independent parts, one for each index of `shift`. The reference program is written for one: setup_inputs(seed, part) draws one part's arguments, and reference() takes and returns one part's arrays. A program takes and returns all parts, laid end to end along the dimension named above; each array names one. Nothing has to cross between parts.
All inputs are finite; a program needn't handle non-finite values.
Results may differ from the reference program's by a relative error of at most 0.001.
Values may be sent and summed in bfloat16 or wider, within the bound.
A program may use at most 192 MiB of HBM per device.

```python
import jax
import jax.numpy as jnp

D_MODEL = 3584
D_INNER = 14336
RANK = 64


def shard_levels(rng, shape, shards, least, top_value):
    gain = 1.0
    for dim, blocks in shards:
        steps = jax.random.uniform(jax.random.fold_in(jax.random.fold_in(rng, 6), dim), (blocks,), jnp.float32, least / len(shards), top_value / len(shards))
        gain = gain * jnp.repeat(jnp.exp(steps), shape[dim] // blocks).reshape((-1,) + (1,) * (len(shape) - 1 - dim))
    return gain


def noise(rng, extent, deviation, reach, shards=(), dtype=jnp.bfloat16):
    array = deviation * jax.random.normal(rng, extent, jnp.float32)
    if shards:
        array = array * shard_levels(rng, extent, shards, -0.22, 0.18)
    return jnp.clip(array, -reach, reach).astype(dtype)


def setup_inputs(seed: int = 0, part: int = 0) -> dict:
    key_list = jax.random.split(jax.random.key(seed), 12)
    part_keys = jax.random.split(jax.random.fold_in(key_list[11], part), 12)
    return {
        "train_gate": noise(part_keys[0], (D_MODEL, D_INNER), D_MODEL ** -0.5, 0.09375, ((0, 2), (1, 8))),
        "low_gate": noise(part_keys[1], (D_MODEL, RANK), D_MODEL ** -0.5, 0.09375, ((0, 2),)),
        "high_gate": noise(part_keys[2], (RANK, D_INNER), RANK ** -0.5, 0.75, ((1, 8),)),
        "train_up": noise(part_keys[3], (D_MODEL, D_INNER), D_MODEL ** -0.5, 0.09375, ((0, 2), (1, 8))),
        "low_up": noise(part_keys[4], (D_MODEL, RANK), D_MODEL ** -0.5, 0.09375, ((0, 2),)),
        "high_up": noise(part_keys[5], (RANK, D_INNER), RANK ** -0.5, 0.75, ((1, 8),)),
        "train_down": noise(part_keys[6], (D_INNER, D_MODEL), D_INNER ** -0.5, 0.046875, ((0, 8), (1, 2))),
        "low_down": noise(part_keys[7], (D_INNER, RANK), D_INNER ** -0.5, 0.046875, ((0, 8),)),
        "high_down": noise(part_keys[8], (RANK, D_MODEL), RANK ** -0.5, 0.75, ((1, 2),)),
        "norm_train": jnp.clip(1.0 + 0.15 * jax.random.normal(part_keys[9], (D_MODEL,), jnp.float32), 0.25, 1.75),
        "norm_step": jnp.clip(jax.random.uniform(part_keys[10], (D_MODEL,), jnp.float32, -0.3, 0.3) * shard_levels(part_keys[10], (D_MODEL,), ((0, 16),), -0.4, 0.0), -0.3, 0.3),
    }


mix_rate = 1.0


def reference(train_gate, low_gate, high_gate, train_up, low_up, high_up, train_down, low_down, high_down, norm_train, norm_step):
    whole_gate = train_gate.astype(jnp.float32) + mix_rate * jnp.dot(low_gate, high_gate, preferred_element_type=jnp.float32)
    whole_up = train_up.astype(jnp.float32) + mix_rate * jnp.dot(low_up, high_up, preferred_element_type=jnp.float32)
    whole_down = train_down.astype(jnp.float32) + mix_rate * jnp.dot(low_down, high_down, preferred_element_type=jnp.float32)
    serving_gate = whole_gate.T.astype(jnp.bfloat16)
    serving_up = whole_up.T.astype(jnp.bfloat16)
    serving_down = whole_down.T.astype(jnp.bfloat16)
    serve_norm = (norm_train + norm_step).astype(jnp.bfloat16)
    return serving_gate, serving_up, serving_down, serve_norm
```

```python
import functools

import jax
import jax.numpy as jnp
from jax import lax
from jax.experimental import pallas as pl
from jax.experimental.pallas import tpu as pltpu
from jax.sharding import PartitionSpec as P


mix_rate = 1.0


def merge_body(train_ref, low_ref, high_ref, *rest):
    send_ref, out_ref = rest[-2:]
    whole = train_ref[...].astype(jnp.float32) + mix_rate * lax.dot_general(
        low_ref[...],
        high_ref[...],
        (((0,), (0,)), ((), ())),
        preferred_element_type=jnp.float32,
    )
    narrow = whole.astype(jnp.bfloat16)
    send_ref[...] = narrow
    out_ref[...] = narrow.T


def merge_chunk(train, low, high, out, before, out_shape, first, count, tile, place):
    width = train.shape[1]
    rank = low.shape[0]
    rows = count * tile
    in_specs = [
        pl.BlockSpec((tile, width), lambda i: (first + i, 0)),
        pl.BlockSpec((rank, tile), lambda i: (0, first + i)),
        pl.BlockSpec((rank, width), lambda i: (0, 0)),
    ]
    args = [train, low, high]
    aliases = {}
    if out is not None:
        in_specs.append(pl.BlockSpec(memory_space=pl.ANY))
        args.append(out)
        aliases = {3: 1}
    if before is not None:
        in_specs.append(pl.BlockSpec(memory_space=pl.ANY))
        args.append(before)
    return pl.pallas_call(
        merge_body,
        grid=(count,),
        in_specs=in_specs,
        out_specs=(
            pl.BlockSpec((tile, width), lambda i: (i, 0)),
            pl.BlockSpec((width, tile), lambda i: place(lax.axis_index("rows"), first + i)),
        ),
        out_shape=(
            jax.ShapeDtypeStruct((rows, width), jnp.bfloat16),
            jax.ShapeDtypeStruct(out_shape, jnp.bfloat16),
        ),
        input_output_aliases=aliases,
        compiler_params=pltpu.CompilerParams(vmem_limit_bytes=67_043_328),
        cost_estimate=pl.CostEstimate(
            flops=2 * rows * rank * width, bytes_accessed=6 * rows * width, transcendentals=0
        ),
    )(*args)


def turn_body(chunk_ref, *rest):
    out_ref = rest[-1]
    out_ref[...] = chunk_ref[...].T


def turn_chunk(chunk, out, before, first, shift, n, tile, place):
    rows, width = chunk.shape

    def where(i):
        source = lax.rem(lax.axis_index("rows") + (n - shift), n)
        return place(source, first + i)

    return pl.pallas_call(
        turn_body,
        grid=(rows // tile,),
        in_specs=[
            pl.BlockSpec((tile, width), lambda i: (i, 0)),
            pl.BlockSpec(memory_space=pl.ANY),
            pl.BlockSpec(memory_space=pl.ANY),
        ],
        out_specs=pl.BlockSpec((width, tile), where),
        out_shape=jax.ShapeDtypeStruct(out.shape, jnp.bfloat16),
        input_output_aliases={1: 0},
        compiler_params=pltpu.CompilerParams(vmem_limit_bytes=67_043_328),
        cost_estimate=pl.CostEstimate(
            flops=0, bytes_accessed=4 * rows * width, transcendentals=0
        ),
    )(chunk, out, before)


def tile_of(rows):
    return 256 if rows % 256 == 0 else 128


def send(chunk, n):
    return [
        lax.ppermute(chunk, "rows", [(d, (d + s) % n) for d in range(n)]) for s in range(1, n)
    ]


def local(
    n,
    train_gate,
    low_gate,
    high_gate,
    train_up,
    low_up,
    high_up,
    train_down,
    low_down,
    high_down,
    norm_train,
    norm_step,
):
    def side(train, low, high):
        rows, width = train.shape
        tile = tile_of(rows)
        tiles = rows // tile
        return train, low.T, high, (width, n * rows), lambda d, t: (0, d * tiles + t)

    def stack(train, low, high):
        rows, width = train.shape
        return train, low.T, high, (n * width, rows), lambda d, t: (d, t)

    matrices = (
        side(train_gate, low_gate, high_gate),
        side(train_up, low_up, high_up),
        stack(train_down, low_down, high_down),
    )
    outs = [None] * 3
    pending = []
    chunk = None
    for m, (train, low, high, shape, place) in enumerate(matrices):
        tile = tile_of(train.shape[0])
        tiles = train.shape[0] // tile
        if m == 0:
            counts = (1, tiles - 1)
        elif m == 1:
            counts = (tiles,)
        else:
            counts = (tiles - 1, 1)
        first = 0
        for count in counts:
            if count == 0:
                continue
            chunk, outs[m] = merge_chunk(
                train, low, high, outs[m], chunk, shape, first, count, tile, place
            )
            pending.append((m, first, tile, place, send(chunk, n)))
            first += count
    norm_train, norm_step, before = lax.optimization_barrier((norm_train, norm_step, chunk))
    serve_norm = lax.all_gather(
        (norm_train + norm_step).astype(jnp.bfloat16), ("rows", "cols"), axis=0, tiled=True
    )
    before, last = chunk, None
    for m, first, tile, place, arrivals in pending:
        for s, chunk in enumerate(arrivals, 1):
            if m == last:
                before = chunk
            outs[m] = before = turn_chunk(chunk, outs[m], before, first, s, n, tile, place)
            last = m
    return (*outs, serve_norm)


def plain(
    train_gate,
    low_gate,
    high_gate,
    train_up,
    low_up,
    high_up,
    train_down,
    low_down,
    high_down,
    norm_train,
    norm_step,
):
    def merged(train, low, high):
        whole = train.astype(jnp.float32) + mix_rate * jnp.dot(
            low, high, preferred_element_type=jnp.float32
        )
        return whole.astype(jnp.bfloat16)

    gather = functools.partial(lax.all_gather, axis_name="rows", tiled=True)
    return (
        gather(merged(train_gate, low_gate, high_gate), axis=0).T,
        gather(merged(train_up, low_up, high_up), axis=0).T,
        gather(merged(train_down, low_down, high_down), axis=1).T,
        lax.all_gather(
            (norm_train + norm_step).astype(jnp.bfloat16), ("rows", "cols"), axis=0, tiled=True
        ),
    )


def body(n, *args):
    sides = args[0].shape + args[3].shape + args[6].shape
    if any(side % 128 for side in sides):
        return plain(*args)
    return local(n, *args)


def solution(mesh):
    return jax.shard_map(
        functools.partial(body, mesh.shape["rows"]),
        mesh=mesh,
        in_specs=(
            P(("shift", "rows"), "cols"),
            P(("shift", "rows"), None),
            P("shift", "cols"),
            P(("shift", "rows"), "cols"),
            P(("shift", "rows"), None),
            P("shift", "cols"),
            P(("shift", "cols"), "rows"),
            P(("shift", "cols"), None),
            P("shift", "rows"),
            P(("shift", "rows", "cols")),
            P(("shift", "rows", "cols")),
        ),
        out_specs=(
            P(("shift", "cols"), None),
            P(("shift", "cols"), None),
            P("shift", "cols"),
            P("shift"),
        ),
        check_vma=False,
    )
```

```python
import functools

import jax
import jax.numpy as jnp
from jax import lax
from jax.experimental import pallas as pl
from jax.experimental.pallas import tpu as pltpu
from jax.sharding import PartitionSpec as P


mix_rate = 1.0
TILE = 128


def merged(train_ref, low_ref, high_ref):
    whole = train_ref[...].astype(jnp.float32) + mix_rate * lax.dot_general(
        low_ref[...],
        high_ref[...],
        (((0,), (0,)), ((), ())),
        preferred_element_type=jnp.float32,
    )
    return whole.astype(jnp.bfloat16)


def merge_body(train_ref, low_ref, high_ref, *rest):
    send_ref, out_ref = rest[-2:]
    narrow = merged(train_ref, low_ref, high_ref)
    send_ref[...] = narrow
    out_ref[...] = narrow.T


def head_body(train_ref, low_ref, high_ref, send_ref):
    send_ref[...] = merged(train_ref, low_ref, high_ref)


def head_chunk(train, low, high, tile):
    width = train.shape[1]
    rank = low.shape[0]
    return pl.pallas_call(
        head_body,
        grid=(1,),
        in_specs=[
            pl.BlockSpec((tile, width), lambda i: (0, 0)),
            pl.BlockSpec((rank, tile), lambda i: (0, 0)),
            pl.BlockSpec((rank, width), lambda i: (0, 0)),
        ],
        out_specs=pl.BlockSpec((tile, width), lambda i: (0, 0)),
        out_shape=jax.ShapeDtypeStruct((tile, width), jnp.bfloat16),
        compiler_params=pltpu.CompilerParams(vmem_limit_bytes=67_043_328),
        cost_estimate=pl.CostEstimate(
            flops=2 * tile * rank * width, bytes_accessed=4 * tile * width, transcendentals=0
        ),
    )(train, low, high)


def merge_chunk(train, low, high, out, before, out_shape, first, count, tile, place):
    width = train.shape[1]
    rank = low.shape[0]
    rows = count * tile
    in_specs = [
        pl.BlockSpec((tile, width), lambda i: (first + i, 0)),
        pl.BlockSpec((rank, tile), lambda i: (0, first + i)),
        pl.BlockSpec((rank, width), lambda i: (0, 0)),
    ]
    args = [train, low, high]
    aliases = {}
    if out is not None:
        in_specs.append(pl.BlockSpec(memory_space=pl.ANY))
        args.append(out)
        aliases = {3: 1}
    if before is not None:
        in_specs.append(pl.BlockSpec(memory_space=pl.ANY))
        args.append(before)
    return pl.pallas_call(
        merge_body,
        grid=(count,),
        in_specs=in_specs,
        out_specs=(
            pl.BlockSpec((tile, width), lambda i: (i, 0)),
            pl.BlockSpec((width, tile), lambda i: place(lax.axis_index("rows"), first + i)),
        ),
        out_shape=(
            jax.ShapeDtypeStruct((rows, width), jnp.bfloat16),
            jax.ShapeDtypeStruct(out_shape, jnp.bfloat16),
        ),
        input_output_aliases=aliases,
        compiler_params=pltpu.CompilerParams(vmem_limit_bytes=67_043_328),
        cost_estimate=pl.CostEstimate(
            flops=2 * rows * rank * width, bytes_accessed=6 * rows * width, transcendentals=0
        ),
    )(*args)


def turn_body(chunk_ref, *rest):
    out_ref = rest[-1]
    out_ref[...] = chunk_ref[...].T


def turn_chunk(chunk, out, before, first, shift, n, tile, place, vmem=64_000_000):
    rows, width = chunk.shape
    args = (chunk, out) if before is None else (chunk, out, before)

    def where(i):
        source = lax.rem(lax.axis_index("rows") + n - shift, n)
        return place(source, first + i)

    return pl.pallas_call(
        turn_body,
        grid=(rows // tile,),
        in_specs=[
            pl.BlockSpec((tile, width), lambda i: (i, 0)),
            *[pl.BlockSpec(memory_space=pl.ANY)] * (len(args) - 1),
        ],
        out_specs=pl.BlockSpec((width, tile), where),
        out_shape=jax.ShapeDtypeStruct(out.shape, jnp.bfloat16),
        input_output_aliases={1: 0},
        compiler_params=pltpu.CompilerParams(vmem_limit_bytes=vmem),
        cost_estimate=pl.CostEstimate(
            flops=0, bytes_accessed=4 * rows * width, transcendentals=0
        ),
    )(*args)


def send(chunk, n):
    return [
        lax.ppermute(chunk, "rows", [(d, (d + s) % n) for d in range(n)]) for s in range(1, n)
    ]


def local(
    n,
    train_gate,
    low_gate,
    high_gate,
    train_up,
    low_up,
    high_up,
    train_down,
    low_down,
    high_down,
    norm_train,
    norm_step,
):
    tile = TILE

    def side(train, low, high):
        rows, width = train.shape
        tiles = rows // tile
        return train, low.T, high, (width, n * rows), lambda d, t: (0, d * tiles + t)

    def stack(train, low, high):
        rows, width = train.shape
        return train, low.T, high, (n * width, rows), lambda d, t: (d, t)

    matrices = (
        side(train_gate, low_gate, high_gate),
        side(train_up, low_up, high_up),
        stack(train_down, low_down, high_down),
    )
    outs = [None] * 3
    pending = []
    chunk = head = None
    for m, (train, low, high, shape, place) in enumerate(matrices):
        tiles = train.shape[0] // tile
        if m == 0:
            cuts = (0, 1, 1 + (tiles - 1) // 3, tiles)
        elif m == 1:
            cuts = (0, tiles)
        else:
            cuts = (0, max(tiles - 3, 0), max(tiles - 1, 0), tiles)
        for first, end in zip(cuts, cuts[1:]):
            if first == end:
                continue
            k = len(pending)
            if k == 0:
                chunk = head = head_chunk(train, low, high, tile)
            else:
                chunk, outs[m] = merge_chunk(
                    train, low, high, outs[m], chunk, shape, first, end - first, tile, place
                )
            pending.append((m, first, place, send(chunk, n)))
    norm_train, norm_step, before = lax.optimization_barrier((norm_train, norm_step, chunk))
    serve_norm = lax.all_gather(
        (norm_train + norm_step).astype(jnp.bfloat16), ("rows", "cols"), axis=0, tiled=True
    )
    outs[0] = turn_chunk(head, outs[0], chunk, 0, 0, n, tile, matrices[0][4])
    last = 0
    for k, (m, first, place, arrivals) in enumerate(pending):
        vmem = 32_000_000 if k == len(pending) - 1 else 64_000_000
        before = None if m == last else outs[last]
        for s, chunk in enumerate(arrivals, 1):
            outs[m] = turn_chunk(chunk, outs[m], before, first, s, n, tile, place, vmem)
            before, last = None, m
    return (*outs, serve_norm)


def plain(
    train_gate,
    low_gate,
    high_gate,
    train_up,
    low_up,
    high_up,
    train_down,
    low_down,
    high_down,
    norm_train,
    norm_step,
):
    def merged(train, low, high):
        whole = train.astype(jnp.float32) + mix_rate * jnp.dot(
            low, high, preferred_element_type=jnp.float32
        )
        return whole.astype(jnp.bfloat16)

    gather = functools.partial(lax.all_gather, axis_name="rows", tiled=True)
    return (
        gather(merged(train_gate, low_gate, high_gate), axis=0).T,
        gather(merged(train_up, low_up, high_up), axis=0).T,
        gather(merged(train_down, low_down, high_down), axis=1).T,
        lax.all_gather(
            (norm_train + norm_step).astype(jnp.bfloat16), ("rows", "cols"), axis=0, tiled=True
        ),
    )


def body(n, *args):
    sides = args[0].shape + args[3].shape + args[6].shape
    if any(side % 128 for side in sides):
        return plain(*args)
    return local(n, *args)


def solution(mesh):
    return jax.shard_map(
        functools.partial(body, mesh.shape["rows"]),
        mesh=mesh,
        in_specs=(
            P(("shift", "rows"), "cols"),
            P(("shift", "rows"), None),
            P("shift", "cols"),
            P(("shift", "rows"), "cols"),
            P(("shift", "rows"), None),
            P("shift", "cols"),
            P(("shift", "cols"), "rows"),
            P(("shift", "cols"), None),
            P("shift", "rows"),
            P(("shift", "rows", "cols")),
            P(("shift", "rows", "cols")),
        ),
        out_specs=(
            P(("shift", "cols"), None),
            P(("shift", "cols"), None),
            P("shift", "cols"),
            P("shift"),
        ),
        check_vma=False,
    )
```
